32 devices in a mesh: dp: 4 (over x, y), tp: 8 (over z, core).
Axes of the slice: x: 2, y: 2, z: 4, core: 2. Of those that a mesh axis runs over, the one named last changes fastest.
Arguments:
- x: bfloat16 [8192, 7168], P('dp'), parts along dimension 0
- w_gate: bfloat16 [7168, 20480], P(None, 'tp')
- w_up: bfloat16 [7168, 20480], P(None, 'tp')
- w_down: bfloat16 [20480, 7168], P('tp')
Outputs:
- output: bfloat16 [8192, 7168], P('dp'), parts along dimension 0
There are 4 independent parts. The reference program is written for one: setup_inputs(seed, part) draws one part's arguments, and reference() takes and returns one part's arrays. A program takes and returns all parts, laid end to end along the dimension named above; an argument that names none is the same for every part.
All inputs are finite; a program needn't handle non-finite values.
Results may differ from the reference program's by a relative error of at most 0.016.
Values are sent between devices in bfloat16 or wider.
A program may use at most 2 GiB of HBM per device.

```python
import jax
import jax.numpy as jnp

ROWS = 2048
D = 7168
FF = 20480


def setup_inputs(seed: int = 0, part: int = 0) -> dict:
    kx, kg, ku, kd = jax.random.split(jax.random.key(seed), 4)
    drawn = {
        "x": jax.random.normal(jax.random.fold_in(kx, part), (ROWS, D), jnp.float32),
        "w_gate": jax.random.normal(kg, (D, FF), jnp.float32) * D**-0.5,
        "w_up": jax.random.normal(ku, (D, FF), jnp.float32) * D**-0.5,
        "w_down": jax.random.normal(kd, (FF, D), jnp.float32) * FF**-0.5,
    }
    return {k: v.astype(jnp.bfloat16) for k, v in drawn.items()}


def reference(x, w_gate, w_up, w_down):
    gate = jnp.dot(x, w_gate, preferred_element_type=jnp.float32)
    up = jnp.dot(x, w_up, preferred_element_type=jnp.float32)
    hidden = (jax.nn.silu(gate) * up).astype(jnp.bfloat16)
    return jnp.dot(hidden, w_down, preferred_element_type=jnp.float32).astype(jnp.bfloat16)
```

```python
import functools

import jax
import jax.numpy as jnp
from jax import lax
from jax.experimental import pallas as pl
from jax.experimental.pallas import tpu as pltpu
from jax.sharding import PartitionSpec as P

MESH = pl.DeviceIdType.MESH
R = 512
TF = 256
TN = 512
KD = 6
KH = 14
KM = 6
KY = 6
LAG_Y = 2
LAG_O = 6


def kernel(chunks, nf, nt, x_hbm, wg_hbm, wu_hbm, wd_hbm, y_hbm,
           xb, wgb, wub, hid, wdb, sb, d1s, d1r, snd, h1r, h2r, yb,
           x_sem, w_sem, wd_sem, d1_ss, d1_rs, snd_ss, h1_rs, h2_rs, yl_sem, y3_ss, y3_rs, y2_ss, y2_rs,
           cr_d1, cr_h1, cr_h2):
    half = R // 2
    total = chunks * nt
    me = lax.axis_index("tp")
    core = lax.rem(me, 2)
    z = me // 2
    partner = me + 1 - 2 * core
    nbr = (z + 1 - 2 * lax.rem(z, 2)) * 2 + core
    mid = (3 - z) * 2 + core
    inner = jnp.logical_or(z == 1, z == 2)
    outer = jnp.logical_not(inner)

    barrier = pltpu.get_barrier_semaphore()
    pl.semaphore_signal(barrier, inc=1, device_id={"tp": partner}, device_id_type=MESH)
    pl.semaphore_signal(barrier, inc=1, device_id={"tp": nbr}, device_id_type=MESH)

    @pl.when(inner)
    def _():
        pl.semaphore_signal(barrier, inc=1, device_id={"tp": mid}, device_id_type=MESH)
        pl.semaphore_wait(barrier, 3)

    @pl.when(outer)
    def _():
        pl.semaphore_wait(barrier, 2)

    def x_copy(c):
        return pltpu.make_async_copy(x_hbm.at[pl.ds(pl.multiple_of(c * R, R), R), :], xb, x_sem)

    def gu_copies(i, slot):
        cols = pl.ds(pl.multiple_of(i * TF, TF), TF)
        return (
            pltpu.make_async_copy(wg_hbm.at[:, cols], wgb.at[slot], w_sem.at[0, slot]),
            pltpu.make_async_copy(wu_hbm.at[:, cols], wub.at[slot], w_sem.at[1, slot]),
        )

    def wd_copy(j, slot):
        cols = pl.ds(pl.multiple_of(j * TN, TN), TN)
        return pltpu.make_async_copy(wd_hbm.at[:, cols], wdb.at[slot], wd_sem.at[slot])

    def region(p, which):
        row = (p // nt) * R + which * half
        return (
            pl.ds(pl.multiple_of(row, half), half),
            pl.ds(pl.multiple_of(lax.rem(p, nt) * TN, TN), TN),
        )

    def remote(src, dst, ss, rs, to):
        return pltpu.make_async_remote_copy(
            src_ref=src, dst_ref=dst, send_sem=ss, recv_sem=rs,
            device_id={"tp": to}, device_id_type=MESH)

    def d1_copy(p):
        k = lax.rem(p, KD)
        return remote(d1s.at[k], d1r.at[k], d1_ss.at[k], d1_rs.at[k], partner)

    def h1_copy(p):
        k = lax.rem(p, KH)
        return remote(snd.at[k], h1r.at[k], snd_ss.at[k], h1_rs.at[k], nbr)

    def h2_copy(p):
        k, m = lax.rem(p, KH), lax.rem(p, KM)
        return remote(snd.at[k], h2r.at[m], snd_ss.at[k], h2_rs.at[m], mid)

    def y_local(p):
        k = lax.rem(p, KY)
        return pltpu.make_async_copy(yb.at[k], y_hbm.at[region(p, core)], yl_sem.at[k])

    def y_out(p):
        k = lax.rem(p, KY)
        return remote(yb.at[k], y_hbm.at[region(p, core)], y3_ss.at[k], y3_rs.at[p], nbr)

    def y_pair(p):
        k = lax.rem(p, KY)
        return remote(yb.at[k], y_hbm.at[region(p, core)], y2_ss.at[p], y2_rs.at[p], partner)

    def y_free(p):
        y_local(p).wait()
        y_out(p).wait_send()
        y_pair(p).wait_send()

    def forward_copy(p):
        at = region(p, core)
        return remote(y_hbm.at[at], y_hbm.at[at], y2_ss.at[p], y2_rs.at[p], partner)

    def produce(p, slot):
        acc = jnp.dot(hid[...], wdb[slot], preferred_element_type=jnp.float32)
        k, s = lax.rem(p, KD), lax.rem(p, KH)

        @pl.when(p >= KD)
        def _():
            d1_copy(p - KD).wait_send()
            pl.semaphore_wait(cr_d1, 1)

        @pl.when(core == 0)
        def _():
            sb[s] = acc[:half]
            d1s[k] = acc[half:].astype(jnp.bfloat16)

        @pl.when(core == 1)
        def _():
            sb[s] = acc[half:]
            d1s[k] = acc[:half].astype(jnp.bfloat16)

        d1_copy(p).start()

    def chip_sum(p):
        k, s = lax.rem(p, KD), lax.rem(p, KH)
        d1_copy(p).wait_recv()

        @pl.when(inner)
        def _():
            sb[s] = sb[s] + d1r[k].astype(jnp.float32)

        @pl.when(outer)
        def _():
            @pl.when(p >= KH)
            def _():
                h1_copy(p - KH).wait_send()
                pl.semaphore_wait(cr_h1, 1)

            snd[s] = (sb[s] + d1r[k].astype(jnp.float32)).astype(jnp.bfloat16)
            h1_copy(p).start()

        @pl.when(p < total - KD)
        def _():
            pl.semaphore_signal(cr_d1, inc=1, device_id={"tp": partner}, device_id_type=MESH)

    def line_sum(p):
        s = lax.rem(p, KH)
        h1_copy(p).wait_recv()
        snd[s] = (sb[s] + h1r[s].astype(jnp.float32)).astype(jnp.bfloat16)

        @pl.when(p < total - KH)
        def _():
            pl.semaphore_signal(cr_h1, inc=1, device_id={"tp": nbr}, device_id_type=MESH)

        @pl.when(p >= KM)
        def _():
            pl.semaphore_wait(cr_h2, 1)

        h2_copy(p).start()

    def finish(p):
        s, m, k = lax.rem(p, KH), lax.rem(p, KM), lax.rem(p, KY)

        @pl.when(p >= KY)
        def _():
            y_free(p - KY)

        h2_copy(p).wait_recv()
        yb[k] = (snd[s].astype(jnp.float32) + h2r[m].astype(jnp.float32)).astype(jnp.bfloat16)
        h2_copy(p).wait_send()

        @pl.when(p < total - KM)
        def _():
            pl.semaphore_signal(cr_h2, inc=1, device_id={"tp": mid}, device_id_type=MESH)

        y_out(p).start()
        y_pair(p).start()
        y_local(p).start()

    def forward(p):
        y_out(p).wait_recv()
        forward_copy(p).start()

    def tick(p):
        @pl.when(inner)
        def _():
            line_sum(p)

            @pl.when(p >= LAG_Y)
            def _():
                finish(p - LAG_Y)

        @pl.when(jnp.logical_and(outer, p >= LAG_O))
        def _():
            forward(p - LAG_O)

    early = 3
    x_copy(0).start()
    for copy in gu_copies(0, 0):
        copy.start()

    def chunk(c, carry):
        base = c * nt
        x_copy(c).wait()

        def gate_up(i, carry):
            slot = lax.rem(i, 2)

            @pl.when(i + 1 < nf)
            def _():
                for copy in gu_copies(i + 1, 1 - slot):
                    copy.start()

            @pl.when(i == nf - 1)
            def _():
                wd_copy(0, 0).start()

            for copy in gu_copies(i, slot):
                copy.wait()
            gate = jnp.dot(xb[...], wgb[slot], preferred_element_type=jnp.float32)
            up = jnp.dot(xb[...], wub[slot], preferred_element_type=jnp.float32)
            hid[:, pl.ds(pl.multiple_of(i * TF, TF), TF)] = (jax.nn.silu(gate) * up).astype(jnp.bfloat16)

            @pl.when(c >= 1)
            def _():
                tick(base - nt + early + i)

            return carry

        lax.fori_loop(0, nf, gate_up, 0)

        @pl.when(c + 1 < chunks)
        def _():
            for copy in gu_copies(0, 0):
                copy.start()

        def down(j, carry):
            p = base + j
            slot = lax.rem(j, 2)

            @pl.when(j + 1 < nt)
            def _():
                wd_copy(j + 1, 1 - slot).start()

            @pl.when(jnp.logical_and(j == 1, c + 1 < chunks))
            def _():
                x_copy(c + 1).start()

            wd_copy(j, slot).wait()
            produce(p, slot)

            @pl.when(j >= 2)
            def _():
                chip_sum(p - 2)

            @pl.when(jnp.logical_and(j == 2, c >= 1))
            def _():
                tick(base - 1)

            @pl.when(j == 8)
            def _():
                tick(base)

            @pl.when(j == 11)
            def _():
                tick(base + 1)

            return carry

        lax.fori_loop(0, nt, down, 0)
        chip_sum(base + nt - 2)
        chip_sum(base + nt - 1)
        tick(base + 2)
        return carry

    lax.fori_loop(0, chunks, chunk, 0)

    def drain(p, carry):
        tick(p)
        return carry

    lax.fori_loop(total - nt + early, total, drain, 0)

    @pl.when(inner)
    def _():
        for p in range(total - LAG_Y, total):
            finish(p)

        def done(p, carry):
            y_free(p)
            return carry

        lax.fori_loop(total - KY, total, done, 0)

    @pl.when(outer)
    def _():
        def late(p, carry):
            forward(p)
            return carry

        lax.fori_loop(total - LAG_O, total, late, 0)

        def sent(p, carry):
            forward_copy(p).wait_send()
            return carry

        lax.fori_loop(0, total, sent, 0)

        def gone(p, carry):
            h1_copy(p).wait_send()
            return carry

        lax.fori_loop(total - KH, total, gone, 0)

    def drained(p, carry):
        d1_copy(p).wait_send()
        return carry

    lax.fori_loop(total - KD, total, drained, 0)

    def arrived(p, carry):
        at = region(p, 1 - core)
        remote(y_hbm.at[at], y_hbm.at[at], y2_ss.at[p], y2_rs.at[p], partner).wait_recv()
        return carry

    lax.fori_loop(0, total, arrived, 0)


def solution(mesh):
    def step(x, w_gate, w_up, w_down):
        rows, d = x.shape
        f = w_gate.shape[1]
        chunks, nf, nt = rows // R, f // TF, d // TN
        total = chunks * nt
        any_ = pl.BlockSpec(memory_space=pl.ANY)
        bf16, dma = jnp.bfloat16, pltpu.SemaphoreType.DMA
        return pl.pallas_call(
            functools.partial(kernel, chunks, nf, nt),
            out_shape=jax.ShapeDtypeStruct((rows, d), bf16),
            in_specs=[any_] * 4,
            out_specs=any_,
            scratch_shapes=[
                pltpu.VMEM((R, d), bf16),
                pltpu.VMEM((2, d, TF), bf16),
                pltpu.VMEM((2, d, TF), bf16),
                pltpu.VMEM((R, f), bf16),
                pltpu.VMEM((2, f, TN), bf16),
                pltpu.VMEM((KH, R // 2, TN), jnp.float32),
                pltpu.VMEM((KD, R // 2, TN), bf16),
                pltpu.VMEM((KD, R // 2, TN), bf16),
                pltpu.VMEM((KH, R // 2, TN), bf16),
                pltpu.VMEM((KH, R // 2, TN), bf16),
                pltpu.VMEM((KM, R // 2, TN), bf16),
                pltpu.VMEM((KY, R // 2, TN), bf16),
                dma, dma((2, 2)), dma((2,)),
                dma((KD,)), dma((KD,)), dma((KH,)), dma((KH,)), dma((KM,)),
                dma((KY,)), dma((KY,)), dma((total,)), dma((total,)), dma((total,)),
                pltpu.SemaphoreType.REGULAR, pltpu.SemaphoreType.REGULAR, pltpu.SemaphoreType.REGULAR,
            ],
            compiler_params=pltpu.CompilerParams(
                collective_id=0, has_side_effects=True, vmem_limit_bytes=67043328),
        )(x, w_gate, w_up, w_down)

    return jax.shard_map(
        step,
        mesh=mesh,
        in_specs=(P("dp", None), P(None, "tp"), P(None, "tp"), P("tp", None)),
        out_specs=P("dp", None),
        check_vma=False,
    )
```

```python
import functools

import jax
import jax.numpy as jnp
from jax import lax
from jax.experimental import pallas as pl
from jax.experimental.pallas import tpu as pltpu
from jax.sharding import PartitionSpec as P

MESH = pl.DeviceIdType.MESH
ROWS = (384, 480, 512, 480, 192)
EARLY = (3, 4, 4, 5, 0)
OWN_AT = ((7, 3), (5, 2), (5, 2), (4, 2), (0, 1))
UNDER = (0, 10, 10, 10, 5)
LATE_AT = ((0, 1), (2, 3), (2, 3), (4, 1), (4, 1))
TF = 256
TN = 512
KD = 5
KS = 6
NW = 3
ND = 2
LAG_Y = 2


def kernel(nf, nt, x_hbm, wg_hbm, wu_hbm, wd_hbm, y_hbm,
           xb, wgb, wub, hid, wdb, sb, d1s, d1r, snd, h1r, h2r, yb,
           x_sem, w_sem, wd_sem, d1_ss, d1_rs, snd_ss, h1_rs, h2_rs, yl_sem, y3_ss, y3_rs, y2_ss, y2_rs,
           cr_d1, cr_h1, cr_h2):
    last = len(ROWS) - 1
    first = [sum(ROWS[:c]) for c in range(last + 1)]
    me = lax.axis_index("tp")
    core = lax.rem(me, 2)
    z = me // 2
    partner = me + 1 - 2 * core
    nbr = (z + 1 - 2 * lax.rem(z, 2)) * 2 + core
    mid = (3 - z) * 2 + core
    inner = jnp.logical_or(z == 1, z == 2)
    outer = jnp.logical_not(inner)

    def x_copy(c):
        return pltpu.make_async_copy(
            x_hbm.at[pl.ds(first[c], ROWS[c]), :], xb.at[pl.ds(0, ROWS[c]), :], x_sem)

    def gu_copies(i):
        slot = lax.rem(i, NW)
        cols = pl.ds(pl.multiple_of(i * TF, TF), TF)
        return (
            pltpu.make_async_copy(wg_hbm.at[:, cols], wgb.at[slot], w_sem.at[0, slot]),
            pltpu.make_async_copy(wu_hbm.at[:, cols], wub.at[slot], w_sem.at[1, slot]),
        )

    def wd_copy(j):
        slot = lax.rem(j, ND)
        cols = pl.ds(pl.multiple_of(j * TN, TN), TN)
        return pltpu.make_async_copy(wd_hbm.at[:, cols], wdb.at[slot], wd_sem.at[slot])

    def part(ref, c, k):
        return ref.at[k, pl.ds(0, ROWS[c] // 2), :]

    def region(c, j, which):
        half = ROWS[c] // 2
        return (
            pl.ds(pl.multiple_of(first[c] + which * half, 16), half),
            pl.ds(pl.multiple_of(j * TN, TN), TN),
        )

    def remote(src, dst, ss, rs, to):
        return pltpu.make_async_remote_copy(
            src_ref=src, dst_ref=dst, send_sem=ss, recv_sem=rs,
            device_id={"tp": to}, device_id_type=MESH)

    def signal(sem, to):
        pl.semaphore_signal(sem, inc=1, device_id={"tp": to}, device_id_type=MESH)

    def d1_copy(c, j):
        k = lax.rem(c * nt + j, KD)
        return remote(part(d1s, c, k), part(d1r, c, k), d1_ss.at[k], d1_rs.at[k], partner)

    def h1_copy(c, j):
        return remote(part(snd, c, j), part(h1r, c, j), snd_ss.at[j], h1_rs.at[j], nbr)

    def h2_copy(c, j):
        k = lax.rem(c * nt + j, KS)
        return remote(part(snd, c, j), part(h2r, c, k), snd_ss.at[j], h2_rs.at[k], mid)

    def y_local(c, j):
        k = lax.rem(c * nt + j, KS)
        return pltpu.make_async_copy(part(yb, c, k), y_hbm.at[region(c, j, core)], yl_sem.at[k])

    def y_out(c, j):
        k, p = lax.rem(c * nt + j, KS), c * nt + j
        return remote(part(yb, c, k), y_hbm.at[region(c, j, core)], y3_ss.at[k], y3_rs.at[p], nbr)

    def y_pair(c, j):
        k, p = lax.rem(c * nt + j, KS), c * nt + j
        return remote(part(yb, c, k), y_hbm.at[region(c, j, core)], y2_ss.at[p], y2_rs.at[p], partner)

    def y_free(c, j):
        y_local(c, j).wait()
        y_out(c, j).wait_send()
        y_pair(c, j).wait_send()

    def forward_copy(c, j, which):
        p, at = c * nt + j, region(c, j, which)
        return remote(y_hbm.at[at], y_hbm.at[at], y2_ss.at[p], y2_rs.at[p], partner)

    def before(c, j, lag, act):
        if isinstance(j, int):
            if j >= lag:
                act(c, j - lag)
            elif c >= 1:
                act(c - 1, j - lag + nt)
            return

        @pl.when(j >= lag)
        def _():
            act(c, j - lag)

        if c >= 1:
            @pl.when(j < lag)
            def _():
                act(c - 1, j - lag + nt)

    def unless_last(c, j, slots, act):
        if c < last:
            act()
        elif isinstance(j, int):
            if j < nt - slots:
                act()
        else:
            @pl.when(j < nt - slots)
            def _():
                act()

    def produce(c, j):
        half = ROWS[c] // 2
        acc = jnp.dot(hid[pl.ds(0, ROWS[c]), :], wdb[lax.rem(j, ND)], preferred_element_type=jnp.float32)
        k = lax.rem(c * nt + j, KD)

        def free(c, j):
            d1_copy(c, j).wait_send()
            pl.semaphore_wait(cr_d1, 1)

        before(c, j, KD, free)

        @pl.when(core == 0)
        def _():
            sb[j, pl.ds(0, half), :] = acc[:half]
            d1s[k, pl.ds(0, half), :] = acc[half:].astype(jnp.bfloat16)

        @pl.when(core == 1)
        def _():
            sb[j, pl.ds(0, half), :] = acc[half:]
            d1s[k, pl.ds(0, half), :] = acc[:half].astype(jnp.bfloat16)

        d1_copy(c, j).start()

    def chip_sum(c, j):
        half = ROWS[c] // 2
        k = lax.rem(c * nt + j, KD)
        d1_copy(c, j).wait_recv()

        @pl.when(inner)
        def _():
            sb[j, pl.ds(0, half), :] = sb[j, pl.ds(0, half), :] + d1r[k, pl.ds(0, half), :].astype(jnp.float32)

        @pl.when(outer)
        def _():
            if c >= 1:
                h1_copy(c - 1, j).wait_send()
                pl.semaphore_wait(cr_h1, 1)
            total = sb[j, pl.ds(0, half), :] + d1r[k, pl.ds(0, half), :].astype(jnp.float32)
            snd[j, pl.ds(0, half), :] = total.astype(jnp.bfloat16)
            h1_copy(c, j).start()

        unless_last(c, j, KD, lambda: signal(cr_d1, partner))

    def line_sum(c, j):
        half = ROWS[c] // 2
        h1_copy(c, j).wait_recv()
        total = sb[j, pl.ds(0, half), :] + h1r[j, pl.ds(0, half), :].astype(jnp.float32)
        snd[j, pl.ds(0, half), :] = total.astype(jnp.bfloat16)
        unless_last(c, j, nt, lambda: signal(cr_h1, nbr))
        before(c, j, KS, lambda c, j: pl.semaphore_wait(cr_h2, 1))
        h2_copy(c, j).start()

    def finish(c, j):
        half = ROWS[c] // 2
        k = lax.rem(c * nt + j, KS)
        before(c, j, KS, y_free)
        h2_copy(c, j).wait_recv()
        total = snd[j, pl.ds(0, half), :].astype(jnp.float32) + h2r[k, pl.ds(0, half), :].astype(jnp.float32)
        yb[k, pl.ds(0, half), :] = total.astype(jnp.bfloat16)
        y_out(c, j).start()
        y_pair(c, j).start()
        y_local(c, j).start()
        h2_copy(c, j).wait_send()
        unless_last(c, j, KS, lambda: signal(cr_h2, mid))

    def forward(c, j):
        y_out(c, j).wait_recv()
        forward_copy(c, j, core).start()

    def tick(c, j):
        @pl.when(inner)
        def _():
            line_sum(c, j)
            before(c, j, LAG_Y, finish)

        @pl.when(outer)
        def _():
            if c >= 1:
                forward(c - 1, j)

    def loop(lo, hi, body):
        def step(i, carry):
            body(i)
            return carry

        lax.fori_loop(lo, hi, step, 0)

    x_copy(0).start()
    for i in range(2):
        for copy in gu_copies(i):
            copy.start()

    barrier = pltpu.get_barrier_semaphore()
    signal(barrier, partner)
    signal(barrier, nbr)

    @pl.when(inner)
    def _():
        signal(barrier, mid)
        pl.semaphore_wait(barrier, 3)

    @pl.when(outer)
    def _():
        pl.semaphore_wait(barrier, 2)

    for c in range(last + 1):
        x_copy(c).wait()
        under = UNDER[c]
        late = nt - EARLY[c - 1] - under if c >= 1 else 0

        def gate_up(i):
            @pl.when(i + 2 < nf)
            def _():
                for copy in gu_copies(i + 2):
                    copy.start()

            @pl.when(i == nf - 1)
            def _():
                wd_copy(0).start()

            for copy in gu_copies(i):
                copy.wait()
            slot = lax.rem(i, NW)
            x = xb[pl.ds(0, ROWS[c]), :]
            gate = jnp.dot(x, wgb[slot], preferred_element_type=jnp.float32)
            up = jnp.dot(x, wub[slot], preferred_element_type=jnp.float32)
            cols = pl.ds(pl.multiple_of(i * TF, TF), TF)
            hid[pl.ds(0, ROWS[c]), cols] = (jax.nn.silu(gate) * up).astype(jnp.bfloat16)
            if under:
                at = EARLY[c - 1]
                loop(at + (i * under) // nf, at + ((i + 1) * under) // nf, lambda j: tick(c - 1, j))

        loop(0, nf, gate_up)

        def down(j):
            @pl.when(j + 1 < nt)
            def _():
                wd_copy(j + 1).start()

            if c < last:
                @pl.when(j == 4)
                def _():
                    x_copy(c + 1).start()

                for i in range(2):
                    @pl.when(j == 2 + 4 * i)
                    def _():
                        for copy in gu_copies(i):
                            copy.start()

            wd_copy(j).wait()
            produce(c, j)

            @pl.when(j >= 2)
            def _():
                chip_sum(c, j - 2)

            def spaced(at, count, act):
                start, gap = at

                @pl.when(jnp.logical_and(
                    jnp.logical_and(j >= start, j <= start + (count - 1) * gap), lax.rem(j - start + gap * nt, gap) == 0))
                def _():
                    act((j - start) // gap)

            if late:
                spaced(LATE_AT[c], late, lambda k: tick(c - 1, nt - late + k))
            if EARLY[c]:
                spaced(OWN_AT[c], EARLY[c], lambda k: tick(c, k))

        loop(0, nt, down)
        chip_sum(c, nt - 2)
        chip_sum(c, nt - 1)

    loop(EARLY[last], nt, lambda j: tick(last, j))

    @pl.when(inner)
    def _():
        loop(nt - LAG_Y, nt, lambda j: finish(last, j))
        loop(nt - KS, nt, lambda j: y_free(last, j))

    @pl.when(outer)
    def _():
        loop(0, nt, lambda j: forward(last, j))
        for c in range(last + 1):
            loop(0, nt, lambda j: forward_copy(c, j, core).wait_send())
        loop(0, nt, lambda j: h1_copy(last, j).wait_send())

    loop(nt - KD, nt, lambda j: d1_copy(last, j).wait_send())
    for c in range(last + 1):
        loop(0, nt, lambda j: forward_copy(c, j, 1 - core).wait_recv())


def solution(mesh):
    def step(x, w_gate, w_up, w_down):
        rows, d = x.shape
        f = w_gate.shape[1]
        nf, nt = f // TF, d // TN
        total = len(ROWS) * nt
        top = max(ROWS)
        any_ = pl.BlockSpec(memory_space=pl.ANY)
        bf16, dma, regular = jnp.bfloat16, pltpu.SemaphoreType.DMA, pltpu.SemaphoreType.REGULAR
        return pl.pallas_call(
            functools.partial(kernel, nf, nt),
            out_shape=jax.ShapeDtypeStruct((rows, d), bf16),
            in_specs=[any_] * 4,
            out_specs=any_,
            scratch_shapes=[
                pltpu.VMEM((top, d), bf16),
                pltpu.VMEM((NW, d, TF), bf16),
                pltpu.VMEM((NW, d, TF), bf16),
                pltpu.VMEM((top, f), bf16),
                pltpu.VMEM((ND, f, TN), bf16),
                pltpu.VMEM((nt, top // 2, TN), jnp.float32),
                pltpu.VMEM((KD, top // 2, TN), bf16),
                pltpu.VMEM((KD, top // 2, TN), bf16),
                pltpu.VMEM((nt, top // 2, TN), bf16),
                pltpu.VMEM((nt, top // 2, TN), bf16),
                pltpu.VMEM((KS, top // 2, TN), bf16),
                pltpu.VMEM((KS, top // 2, TN), bf16),
                dma, dma((2, NW)), dma((ND,)),
                dma((KD,)), dma((KD,)), dma((nt,)), dma((nt,)), dma((KS,)),
                dma((KS,)), dma((KS,)), dma((total,)), dma((total,)), dma((total,)),
                regular, regular, regular,
            ],
            compiler_params=pltpu.CompilerParams(
                collective_id=0, has_side_effects=True, vmem_limit_bytes=67043328),
        )(x, w_gate, w_up, w_down)

    return jax.shard_map(
        step,
        mesh=mesh,
        in_specs=(P("dp", None), P(None, "tp"), P(None, "tp"), P("tp", None)),
        out_specs=P("dp", None),
        check_vma=False,
    )
```

```python
import functools

import jax
import jax.numpy as jnp
from jax import lax
from jax.experimental import pallas as pl
from jax.experimental.pallas import tpu as pltpu
from jax.sharding import PartitionSpec as P

MESH = pl.DeviceIdType.MESH
ROWS = (384, 480, 480, 448, 256)
EARLY = (3, 4, 4, 5, 0)
OWN_AT = ((5, 4), (4, 3), (4, 3), (4, 2), (0, 1))
UNDER = (0, 10, 10, 10, 7)
LATE_AT = ((0, 1), (1, 1), (4, 4), (0, 4), (4, 3))
TF = 256
TN = 512
KD = 4
KS = 5
NW = 3
ND = 3
LAG_Y = 2


def kernel(nf, nt, x_hbm, wg_hbm, wu_hbm, wd_hbm, y_hbm,
           xb, wgb, wub, hid, wdb, sb, d1s, d1r, snd, h1r, h2r, yb,
           x_sem, w_sem, wd_sem, d1_ss, d1_rs, snd_ss, h1_rs, h2_rs, yl_sem, y3_ss, y3_rs, y2_ss, y2_rs,
           cr_d1, cr_h1, cr_h2):
    last = len(ROWS) - 1
    first = [sum(ROWS[:c]) for c in range(last + 1)]
    me = lax.axis_index("tp")
    core = lax.rem(me, 2)
    z = me // 2
    partner = me + 1 - 2 * core
    nbr = (z + 1 - 2 * lax.rem(z, 2)) * 2 + core
    mid = (3 - z) * 2 + core
    inner = jnp.logical_or(z == 1, z == 2)
    outer = jnp.logical_not(inner)

    def x_copy(c):
        return pltpu.make_async_copy(
            x_hbm.at[pl.ds(first[c], ROWS[c]), :], xb.at[pl.ds(0, ROWS[c]), :], x_sem)

    def gu_copies(i):
        slot = lax.rem(i, NW)
        cols = pl.ds(pl.multiple_of(i * TF, TF), TF)
        return (
            pltpu.make_async_copy(wg_hbm.at[:, cols], wgb.at[slot], w_sem.at[0, slot]),
            pltpu.make_async_copy(wu_hbm.at[:, cols], wub.at[slot], w_sem.at[1, slot]),
        )

    def wd_copy(j):
        slot = lax.rem(j, ND)
        cols = pl.ds(pl.multiple_of(j * TN, TN), TN)
        return pltpu.make_async_copy(wd_hbm.at[:, cols], wdb.at[slot], wd_sem.at[slot])

    def part(ref, c, k):
        return ref.at[k, pl.ds(0, ROWS[c] // 2), :]

    def region(c, j, which):
        half = ROWS[c] // 2
        return (
            pl.ds(pl.multiple_of(first[c] + which * half, 16), half),
            pl.ds(pl.multiple_of(j * TN, TN), TN),
        )

    def remote(src, dst, ss, rs, to):
        return pltpu.make_async_remote_copy(
            src_ref=src, dst_ref=dst, send_sem=ss, recv_sem=rs,
            device_id={"tp": to}, device_id_type=MESH)

    def signal(sem, to):
        pl.semaphore_signal(sem, inc=1, device_id={"tp": to}, device_id_type=MESH)

    def d1_copy(c, j):
        k = lax.rem(c * nt + j, KD)
        return remote(part(d1s, c, k), part(d1r, c, k), d1_ss.at[k], d1_rs.at[k], partner)

    def h1_copy(c, j):
        return remote(part(snd, c, j), part(h1r, c, j), snd_ss.at[j], h1_rs.at[j], nbr)

    def h2_copy(c, j):
        k = lax.rem(c * nt + j, KS)
        return remote(part(snd, c, j), part(h2r, c, k), snd_ss.at[j], h2_rs.at[k], mid)

    def y_local(c, j):
        k = lax.rem(c * nt + j, KS)
        return pltpu.make_async_copy(part(yb, c, k), y_hbm.at[region(c, j, core)], yl_sem.at[k])

    def y_out(c, j):
        k, p = lax.rem(c * nt + j, KS), c * nt + j
        return remote(part(yb, c, k), y_hbm.at[region(c, j, core)], y3_ss.at[k], y3_rs.at[p], nbr)

    def y_pair(c, j):
        k, p = lax.rem(c * nt + j, KS), c * nt + j
        return remote(part(yb, c, k), y_hbm.at[region(c, j, core)], y2_ss.at[p], y2_rs.at[p], partner)

    def y_free(c, j):
        y_local(c, j).wait()
        y_out(c, j).wait_send()
        y_pair(c, j).wait_send()

    def forward_copy(c, j, which):
        p, at = c * nt + j, region(c, j, which)
        return remote(y_hbm.at[at], y_hbm.at[at], y2_ss.at[p], y2_rs.at[p], partner)

    def before(c, j, lag, act):
        if isinstance(j, int):
            if j >= lag:
                act(c, j - lag)
            elif c >= 1:
                act(c - 1, j - lag + nt)
            return

        @pl.when(j >= lag)
        def _():
            act(c, j - lag)

        if c >= 1:
            @pl.when(j < lag)
            def _():
                act(c - 1, j - lag + nt)

    def unless_last(c, j, slots, act):
        if c < last:
            act()
        elif isinstance(j, int):
            if j < nt - slots:
                act()
        else:
            @pl.when(j < nt - slots)
            def _():
                act()

    def produce(c, j):
        half = ROWS[c] // 2
        acc = jnp.dot(hid[pl.ds(0, ROWS[c]), :], wdb[lax.rem(j, ND)], preferred_element_type=jnp.float32)
        k = lax.rem(c * nt + j, KD)

        def free(c, j):
            d1_copy(c, j).wait_send()
            pl.semaphore_wait(cr_d1, 1)

        before(c, j, KD, free)

        @pl.when(core == 0)
        def _():
            sb[j, pl.ds(0, half), :] = acc[:half]
            d1s[k, pl.ds(0, half), :] = acc[half:].astype(jnp.bfloat16)

        @pl.when(core == 1)
        def _():
            sb[j, pl.ds(0, half), :] = acc[half:]
            d1s[k, pl.ds(0, half), :] = acc[:half].astype(jnp.bfloat16)

        d1_copy(c, j).start()

    def chip_sum(c, j):
        half = ROWS[c] // 2
        k = lax.rem(c * nt + j, KD)
        d1_copy(c, j).wait_recv()

        @pl.when(inner)
        def _():
            sb[j, pl.ds(0, half), :] = sb[j, pl.ds(0, half), :] + d1r[k, pl.ds(0, half), :].astype(jnp.float32)

        @pl.when(outer)
        def _():
            if c >= 1:
                h1_copy(c - 1, j).wait_send()
                pl.semaphore_wait(cr_h1, 1)
            total = sb[j, pl.ds(0, half), :] + d1r[k, pl.ds(0, half), :].astype(jnp.float32)
            snd[j, pl.ds(0, half), :] = total.astype(jnp.bfloat16)
            h1_copy(c, j).start()

        unless_last(c, j, KD, lambda: signal(cr_d1, partner))

    def line_sum(c, j):
        half = ROWS[c] // 2
        h1_copy(c, j).wait_recv()
        total = sb[j, pl.ds(0, half), :] + h1r[j, pl.ds(0, half), :].astype(jnp.float32)
        snd[j, pl.ds(0, half), :] = total.astype(jnp.bfloat16)
        unless_last(c, j, nt, lambda: signal(cr_h1, nbr))
        before(c, j, KS, lambda c, j: pl.semaphore_wait(cr_h2, 1))
        h2_copy(c, j).start()

    def finish(c, j):
        half = ROWS[c] // 2
        k = lax.rem(c * nt + j, KS)
        before(c, j, KS, y_free)
        h2_copy(c, j).wait_recv()
        total = snd[j, pl.ds(0, half), :].astype(jnp.float32) + h2r[k, pl.ds(0, half), :].astype(jnp.float32)
        yb[k, pl.ds(0, half), :] = total.astype(jnp.bfloat16)
        y_out(c, j).start()
        y_pair(c, j).start()
        y_local(c, j).start()
        h2_copy(c, j).wait_send()
        unless_last(c, j, KS, lambda: signal(cr_h2, mid))

    def forward(c, j):
        y_out(c, j).wait_recv()
        forward_copy(c, j, core).start()

    def tick(c, j):
        @pl.when(inner)
        def _():
            line_sum(c, j)
            before(c, j, LAG_Y, finish)

        @pl.when(outer)
        def _():
            if c >= 1:
                forward(c - 1, j)

    def loop(lo, hi, body):
        def step(i, carry):
            body(i)
            return carry

        lax.fori_loop(lo, hi, step, 0)

    x_copy(0).start()
    for i in range(2):
        for copy in gu_copies(i):
            copy.start()

    barrier = pltpu.get_barrier_semaphore()
    signal(barrier, partner)
    signal(barrier, nbr)

    @pl.when(inner)
    def _():
        signal(barrier, mid)
        pl.semaphore_wait(barrier, 3)

    @pl.when(outer)
    def _():
        pl.semaphore_wait(barrier, 2)

    for c in range(last + 1):
        x_copy(c).wait()
        under = UNDER[c]
        late = nt - EARLY[c - 1] - under if c >= 1 else 0

        def gate_up(i):
            @pl.when(i + 2 < nf)
            def _():
                for copy in gu_copies(i + 2):
                    copy.start()

            @pl.when(i >= nf - 2)
            def _():
                wd_copy(i - (nf - 2)).start()

            for copy in gu_copies(i):
                copy.wait()
            slot = lax.rem(i, NW)
            x = xb[pl.ds(0, ROWS[c]), :]
            gate = jnp.dot(x, wgb[slot], preferred_element_type=jnp.float32)
            up = jnp.dot(x, wub[slot], preferred_element_type=jnp.float32)
            cols = pl.ds(pl.multiple_of(i * TF, TF), TF)
            hid[pl.ds(0, ROWS[c]), cols] = (jax.nn.silu(gate) * up).astype(jnp.bfloat16)
            if under:
                at = EARLY[c - 1]
                loop(at + (i * under) // nf, at + ((i + 1) * under) // nf, lambda j: tick(c - 1, j))

        loop(0, nf, gate_up)

        def down(j):
            @pl.when(j + 2 < nt)
            def _():
                wd_copy(j + 2).start()

            if c < last:
                @pl.when(j == 4)
                def _():
                    x_copy(c + 1).start()

                for i in range(2):
                    @pl.when(j == 2 + 4 * i)
                    def _():
                        for copy in gu_copies(i):
                            copy.start()

            wd_copy(j).wait()
            produce(c, j)

            @pl.when(j >= 2)
            def _():
                chip_sum(c, j - 2)

            def spaced(at, count, act):
                start, gap = at

                @pl.when(jnp.logical_and(
                    jnp.logical_and(j >= start, j <= start + (count - 1) * gap), lax.rem(j - start + gap * nt, gap) == 0))
                def _():
                    act((j - start) // gap)

            if late:
                spaced(LATE_AT[c], late, lambda k: tick(c - 1, nt - late + k))
            if EARLY[c]:
                spaced(OWN_AT[c], EARLY[c], lambda k: tick(c, k))

        loop(0, nt, down)
        chip_sum(c, nt - 2)
        chip_sum(c, nt - 1)

    loop(EARLY[last], nt, lambda j: tick(last, j))

    @pl.when(inner)
    def _():
        loop(nt - LAG_Y, nt, lambda j: finish(last, j))
        loop(nt - KS, nt, lambda j: y_free(last, j))

    @pl.when(outer)
    def _():
        loop(0, nt, lambda j: forward(last, j))
        for c in range(last + 1):
            loop(0, nt, lambda j: forward_copy(c, j, core).wait_send())
        loop(0, nt, lambda j: h1_copy(last, j).wait_send())

    loop(nt - KD, nt, lambda j: d1_copy(last, j).wait_send())
    for c in range(last + 1):
        loop(0, nt, lambda j: forward_copy(c, j, 1 - core).wait_recv())


def solution(mesh):
    def step(x, w_gate, w_up, w_down):
        rows, d = x.shape
        f = w_gate.shape[1]
        nf, nt = f // TF, d // TN
        total = len(ROWS) * nt
        top = max(ROWS)
        any_ = pl.BlockSpec(memory_space=pl.ANY)
        bf16, dma, regular = jnp.bfloat16, pltpu.SemaphoreType.DMA, pltpu.SemaphoreType.REGULAR
        return pl.pallas_call(
            functools.partial(kernel, nf, nt),
            out_shape=jax.ShapeDtypeStruct((rows, d), bf16),
            in_specs=[any_] * 4,
            out_specs=any_,
            scratch_shapes=[
                pltpu.VMEM((top, d), bf16),
                pltpu.VMEM((NW, d, TF), bf16),
                pltpu.VMEM((NW, d, TF), bf16),
                pltpu.VMEM((top, f), bf16),
                pltpu.VMEM((ND, f, TN), bf16),
                pltpu.VMEM((nt, top // 2, TN), jnp.float32),
                pltpu.VMEM((KD, top // 2, TN), bf16),
                pltpu.VMEM((KD, top // 2, TN), bf16),
                pltpu.VMEM((nt, top // 2, TN), bf16),
                pltpu.VMEM((nt, top // 2, TN), bf16),
                pltpu.VMEM((KS, top // 2, TN), bf16),
                pltpu.VMEM((KS, top // 2, TN), bf16),
                dma, dma((2, NW)), dma((ND,)),
                dma((KD,)), dma((KD,)), dma((nt,)), dma((nt,)), dma((KS,)),
                dma((KS,)), dma((KS,)), dma((total,)), dma((total,)), dma((total,)),
                regular, regular, regular,
            ],
            compiler_params=pltpu.CompilerParams(
                collective_id=0, has_side_effects=True, vmem_limit_bytes=67043328),
        )(x, w_gate, w_up, w_down)

    return jax.shard_map(
        step,
        mesh=mesh,
        in_specs=(P("dp", None), P(None, "tp"), P(None, "tp"), P("tp", None)),
        out_specs=P("dp", None),
        check_vma=False,
    )
```
